32 devices in a mesh: seq: 8 (over z, core), exp: 4 (over y, x).
Axes of the slice: x: 2, y: 2, z: 4, core: 2. Of those that a mesh axis runs over, the one named last changes fastest.
Arguments:
- queries: bfloat16 [768, 4096], P('seq', 'exp'), may hold values from -17 to 17
- keys: bfloat16 [768, 1024], P('seq', 'exp'), may hold values from -17 to 17
- values: bfloat16 [768, 1024], P('seq', 'exp'), may hold values from -6 to 6
- residual: bfloat16 [768, 4096], P('seq', 'exp'), may hold values from -48 to 48
- norm_gain: float32 [4096], P('exp'), may hold values from 0.1 to 1.9
- routes: int32 [768, 2], P('seq'), may hold values from 0 to 3, all different within a row; in each aligned block of 96 rows (0 to 95, 96 to 191, ...) at most 72 rows name the same one
- gates: float32 [768, 2], P('seq'), may hold values from 0.1 to 0.9
- w_gate: bfloat16 [4, 4096, 14336], P('exp', None, 'seq'), may hold values from -0.09375 to 0.09375
- w_up: bfloat16 [4, 4096, 14336], P('exp', None, 'seq'), may hold values from -0.09375 to 0.09375
- w_down: bfloat16 [4, 14336, 4096], P('exp', 'seq'), may hold values from -0.046875 to 0.046875
Outputs:
- attended: bfloat16 [768, 4096], P('seq', 'exp')
- layer_out: bfloat16 [768, 4096], P('seq', 'exp')
The draws below stay inside these ranges and needn't reach their ends.
Inputs may be any that keep to these rules, and one draw needn't show every extreme that they name: `routes`: each row names 2 different experts. In the rows of one device no expert is named more than 72 times, a bound that some block reaches.
All inputs are finite; a program needn't handle non-finite values.
Results may differ from the reference program's by a relative error of at most 0.0075.
Values may be sent and summed in bfloat16 or wider, within the bound.
No kernel may reach another device: no remote copies, remote signals or barrier semaphores. Data moves between devices by JAX's collectives and lax.ppermute only.
A program may use at most 128 MiB of HBM per device.

```python
import math
import jax
import jax.numpy as jnp
import numpy as np
from jax import lax

D = 4096
QUERY_HEADS = 32
KEY_VALUE_HEADS = 8
HEAD_WIDTH = 128
FF = 14336
TOP = 2
TOK_DEV = 96
SEQUENCE_LENGTH = 768
EXPERTS = 4
CAP = 72
N_SEQ = 8


def draw_keys(key, part):
    layer_result = jnp.clip(jax.random.normal(jax.random.fold_in(key, 2), (SEQUENCE_LENGTH, KEY_VALUE_HEADS * HEAD_WIDTH), jnp.float32), -4.0, 4.0)
    layer_result = jnp.clip(layer_result, -16.5, 16.5)
    return layer_result.astype(jnp.bfloat16)


def draw_queries(key, part):
    layer_result = jnp.clip(jax.random.normal(jax.random.fold_in(key, 1), (SEQUENCE_LENGTH, QUERY_HEADS * HEAD_WIDTH), jnp.float32), -4.0, 4.0)
    layer_result = jnp.clip(layer_result, -16.5, 16.5)
    return layer_result.astype(jnp.bfloat16)


def draw_residual(key, part):
    base = jnp.clip(jax.random.normal(jax.random.fold_in(key, 5), (SEQUENCE_LENGTH, D), jnp.float32), -4.0, 4.0)
    column = jnp.arange(D, dtype=jnp.float32) / max(D - 1, 1)
    column_scale = 0.6 * jnp.exp(column * math.log(5.0))
    layer_result = base * column_scale[None, :]
    return layer_result.astype(jnp.bfloat16)


def steps_of(key, extent, shards, smallest, top_value):
    loudness = 1.0
    for axis_at, shards_of in shards:
        steps = jax.random.uniform(jax.random.fold_in(jax.random.fold_in(key, 6), axis_at), (shards_of,), jnp.float32, smallest / len(shards), top_value / len(shards))
        loudness = loudness * jnp.repeat(jnp.exp(steps), extent[axis_at] // shards_of).reshape((-1,) + (1,) * (len(extent) - 1 - axis_at))
    return loudness


def assign_block(key, own, number, rows, amount, top, bound, skew):
    ranking = jax.random.permutation(key, amount)
    packed, common = shares(amount, rows * top, bound, skew, True), shares(amount, rows * top, bound, skew, False)
    places = jnp.arange(amount)

    def named(tallies, offset_by):
        used = int((tallies > 0).sum())
        fixed = max(1, used // 4)
        moved = fixed + (places - fixed + offset_by * (used - fixed)) % max(1, amount - fixed)
        return jnp.zeros((amount,), jnp.int32).at[ranking[jnp.where(places < fixed, places, moved)]].set(jnp.asarray(tallies, jnp.int32))

    tallies = jnp.where(number % 4 == 0, named(packed, number // 4), named(common, number - number // 4 - 1))
    mixed = jax.random.permutation(jax.random.fold_in(own, 3), amount)
    source_of, taker = mixed[0:amount // 2 * 2:2], mixed[1:amount // 2 * 2:2]
    room = jnp.minimum(tallies[source_of] - 1, bound - tallies[taker]) // 2
    room = jnp.where((source_of == ranking[0]) | (taker == ranking[0]) | (tallies[taker] == 0), 0, jnp.maximum(room, 0))
    moved = jax.random.randint(jax.random.fold_in(own, 4), (amount // 2,), 0, 1 << 20) % (room + 1)
    tallies = tallies.at[source_of].add(-moved).at[taker].add(moved)
    labels = jnp.searchsorted(jnp.cumsum(tallies), jnp.arange(rows * top), side="right").astype(jnp.int32)
    grid = labels.reshape(top, rows).T
    grid = grid[jax.random.permutation(jax.random.fold_in(own, 1), rows)]
    offset_by = jax.random.randint(jax.random.fold_in(own, 2), (rows, 1), 0, top)
    return jnp.take_along_axis(grid, (jnp.arange(top)[None, :] + offset_by) % top, axis=1)


def shares(number_of, total, limit, lean, full):
    loads = [(1 << 20) // math.isqrt(rank ** lean) + 1 for rank in range(1, number_of + 1)]
    largest = limit if full else min(limit, max(-(-total // number_of), total * loads[0] // sum(loads)))
    least = 1 if total - largest >= number_of - 1 else 0
    given, rest = [largest] + [least] * (number_of - 1), total - largest - least * (number_of - 1)
    while rest > 0:
        free = [i for i in range(1, number_of) if given[i] < largest] or [i for i in range(1, number_of) if given[i] < limit]
        pool, left = sum([loads[i] for i in free]), rest
        for i in free:
            more = min(limit - given[i], max(1, left * loads[i] // pool), rest)
            given[i] = given[i] + more
            rest = rest - more
    return np.array(given)


def noise(stream_key, extent, deviation, limit, split=(), kind=jnp.bfloat16):
    result = deviation * jax.random.normal(stream_key, extent, jnp.float32)
    if split:
        result = result * steps_of(stream_key, extent, split, -0.22, 0.18)
    return jnp.clip(result, -limit, limit).astype(kind)


def setup_inputs(seed: int = 0) -> dict:
    seeds = jax.random.split(jax.random.key(seed), 11)
    queries = draw_queries(jax.random.fold_in(seeds[10], 71), 0)
    keys = draw_keys(jax.random.fold_in(seeds[10], 71), 0)
    values = noise(seeds[2], (SEQUENCE_LENGTH, KEY_VALUE_HEADS * HEAD_WIDTH), 1.0, 6.0, ((0, 8), (1, 4)))
    residual = draw_residual(jax.random.fold_in(seeds[10], 71), 0)
    norm_gain = jnp.clip(1.0 + 0.18 * jax.random.normal(seeds[4], (D,), jnp.float32), 0.1, 1.9)
    routes_keys = jax.random.split(jax.random.fold_in(seeds[5], 1), SEQUENCE_LENGTH // TOK_DEV)
    routes_turns = jax.random.permutation(jax.random.fold_in(seeds[5], 3), SEQUENCE_LENGTH // TOK_DEV)
    routes = jax.vmap(lambda own, number: assign_block(jax.random.fold_in(seeds[5], 2), own, number, TOK_DEV, EXPERTS, TOP, CAP, 2))(routes_keys, routes_turns).reshape((SEQUENCE_LENGTH, TOP))
    gates = jnp.clip(0.1 + 0.79999997 * jax.random.uniform(seeds[6], (SEQUENCE_LENGTH, TOP), jnp.float32) ** steps_of(seeds[6], (SEQUENCE_LENGTH, TOP), ((0, 8),), -0.2, 0.2), 0.1, 0.9)
    w_gate = noise(seeds[7], (EXPERTS, D, FF), D ** -0.5, 0.09375, ((0, 4), (2, 8)))
    w_up = noise(seeds[8], (EXPERTS, D, FF), D ** -0.5, 0.09375, ((0, 4), (2, 8)))
    w_down = noise(seeds[9], (EXPERTS, FF, D), FF ** -0.5, 0.046875, ((0, 4), (1, 8)))
    return {"queries": queries, "keys": keys, "values": values, "residual": residual, "norm_gain": norm_gain, "routes": routes, "gates": gates, "w_gate": w_gate, "w_up": w_up, "w_down": w_down}


def attend_head(inputs):
    query_head, key_head, value_head = inputs
    scores = jnp.einsum('tgd,pd->gtp', query_head, key_head) / math.sqrt(HEAD_WIDTH)
    positions = jnp.arange(SEQUENCE_LENGTH, dtype=jnp.int32)
    causal_mask = (positions[None, :] <= positions[:, None])[None, :, :]
    scores = jnp.where(causal_mask, scores, -1e+30)
    row_max = lax.optimization_barrier(jnp.max(scores, axis=-1, keepdims=True))
    exp_terms = jnp.where(causal_mask, jnp.exp(scores - row_max), 0.0)
    denominator = lax.optimization_barrier(jnp.sum(exp_terms, axis=-1))
    probs_low = exp_terms.astype(jnp.bfloat16).astype(jnp.float32)
    return jnp.einsum('gtp,pd->gtd', probs_low, value_head) / denominator[..., None]

def expert_apply(inputs):
    rows, gate_mat, up_mat, down_mat = inputs
    hidden = (jax.nn.silu(jnp.dot(rows, gate_mat, preferred_element_type=jnp.float32)) * jnp.dot(rows, up_mat, preferred_element_type=jnp.float32)).astype(jnp.bfloat16)
    row_count = rows.shape[0]
    block_width = FF // N_SEQ
    hidden_blocks = jnp.transpose(hidden.reshape(row_count, N_SEQ, block_width), (1, 0, 2))
    down_blocks = down_mat.reshape(N_SEQ, block_width, D)

    def add_block(total, pair):
        hidden_block, down_block = pair
        term = jnp.dot(hidden_block, down_block, preferred_element_type=jnp.float32).astype(jnp.bfloat16)
        term = lax.optimization_barrier(term)
        return (total + term.astype(jnp.float32), None)
    total, unused = lax.scan(add_block, jnp.zeros((row_count, D), jnp.float32), (hidden_blocks, down_blocks))
    return total.astype(jnp.bfloat16)

def reference(queries, keys, values, residual, norm_gain, routes, gates, w_gate, w_up, w_down):
    group_width = QUERY_HEADS // KEY_VALUE_HEADS
    query_head_rows = jnp.transpose(queries.astype(jnp.float32).reshape(SEQUENCE_LENGTH, KEY_VALUE_HEADS, group_width, HEAD_WIDTH), (1, 0, 2, 3))
    key_head_rows = jnp.transpose(keys.astype(jnp.float32).reshape(SEQUENCE_LENGTH, KEY_VALUE_HEADS, HEAD_WIDTH), (1, 0, 2))
    value_head_rows = jnp.transpose(values.astype(jnp.float32).reshape(SEQUENCE_LENGTH, KEY_VALUE_HEADS, HEAD_WIDTH), (1, 0, 2))
    heads_out = lax.map(attend_head, (query_head_rows, key_head_rows, value_head_rows))
    attn = jnp.transpose(heads_out, (2, 0, 1, 3)).reshape(SEQUENCE_LENGTH, QUERY_HEADS * HEAD_WIDTH)
    attended = (residual.astype(jnp.float32) + attn).astype(jnp.bfloat16)
    stream = attended.astype(jnp.float32)
    mean_square = lax.optimization_barrier(jnp.mean(stream * stream, axis=-1, keepdims=True))
    inverse_root = lax.rsqrt(mean_square + 1e-05)
    normed = (stream * inverse_root * norm_gain.astype(jnp.float32)).astype(jnp.bfloat16)
    blocks = N_SEQ
    assigned = TOK_DEV * TOP
    normed_blocks = normed.reshape(blocks, TOK_DEV, D)
    route_blocks = routes.reshape(blocks, assigned).astype(jnp.int32)
    one_hot = (route_blocks[:, :, None] == jnp.arange(EXPERTS, dtype=jnp.int32)[None, None, :]).astype(jnp.int32)
    before = jnp.cumsum(one_hot, axis=1) - one_hot
    slot_index = lax.optimization_barrier(jnp.sum(before * one_hot, axis=-1)).astype(jnp.int32)
    dest_slot = (route_blocks * CAP + slot_index).astype(jnp.int32)
    selected = (dest_slot[:, :, None] == jnp.arange(EXPERTS * CAP, dtype=jnp.int32)[None, None, :]).astype(jnp.int32)
    token_of = (jnp.arange(assigned, dtype=jnp.int32) // TOP)[None, :, None]
    token_index = lax.optimization_barrier(jnp.sum(selected * token_of, axis=1)).astype(jnp.int32)
    filled = lax.optimization_barrier(jnp.sum(selected, axis=1))
    slot_rows = jnp.take_along_axis(normed_blocks, token_index[:, :, None], axis=1)
    slot_rows = jnp.where(filled[:, :, None] > 0, slot_rows, jnp.zeros_like(slot_rows))
    by_expert = jnp.transpose(slot_rows.reshape(blocks, EXPERTS, CAP, D), (1, 0, 2, 3)).reshape(EXPERTS, blocks * CAP, D)
    expert_out = lax.map(expert_apply, (by_expert, w_gate, w_up, w_down))
    flat_out = expert_out.reshape(EXPERTS * blocks * CAP, D)
    block_ids = jnp.arange(blocks, dtype=jnp.int32)[:, None]
    flat_index = ((route_blocks * blocks + block_ids) * CAP + slot_index).astype(jnp.int32)
    picked = flat_out[flat_index].astype(jnp.float32).reshape(blocks, TOK_DEV, TOP, D)
    gate_blocks = gates.astype(jnp.float32).reshape(blocks, TOK_DEV, TOP)
    mixture = lax.optimization_barrier(jnp.sum(gate_blocks[..., None] * picked, axis=2)).reshape(SEQUENCE_LENGTH, D)
    layer_out = (stream + mixture).astype(jnp.bfloat16)
    return (attended, layer_out)
```

```python
import math

import jax
import jax.numpy as jnp
from jax import lax
from jax.experimental import pallas as pl
from jax.experimental.pallas import tpu as pltpu
from jax.sharding import PartitionSpec as P

D = 4096
QUERY_HEADS = 32
KEY_VALUE_HEADS = 8
HEAD_WIDTH = 128
TOP = 2
CHUNKS = 2


def chip_shift(x, step):
    n = lax.axis_size("seq")
    return lax.ppermute(x, "seq", [(i, (i + 2 * step) % n) for i in range(n)])


def core_swap(x):
    n = lax.axis_size("seq")
    return lax.ppermute(x, "seq", [(i, i ^ 1) for i in range(n)])


def exp_swap(x, k):
    n = lax.axis_size("exp")
    return lax.ppermute(x, "exp", [(i, i ^ k) for i in range(n)])


def low_half(rows):
    return (rows // 2 + 7) // 8 * 8


def gather_seq(x):
    chips = lax.axis_size("seq") // 2
    far = chips // 2
    cut = low_half(x.shape[0])
    blocks = [None] * chips
    blocks[0] = x
    ahead = behind = x
    for d in range(1, far):
        behind = chip_shift(behind, 1)
        ahead = chip_shift(ahead, -1)
        blocks[-d] = behind
        blocks[d] = ahead
    top = chip_shift(behind[:cut], 1)
    bottom = chip_shift(ahead[cut:], -1)
    blocks[far] = jnp.concatenate([top, bottom], axis=0)
    mine = jnp.concatenate(blocks, axis=0)
    other = core_swap(mine)
    return jnp.concatenate([mine, other], axis=0)


def add(a, b):
    return (a.astype(jnp.float32) + b.astype(jnp.float32)).astype(a.dtype)


def reduce_seq(partial):
    n = lax.axis_size("seq")
    chips = n // 2
    far = chips // 2
    half = partial.shape[0] // 2
    rows = half // chips
    cut = low_half(rows)
    other = core_swap(partial[half:])
    both = add(partial[:half], other)
    block = [both[d * rows : (d + 1) * rows] for d in range(chips)]
    top = chip_shift(block[far][:cut], 1)
    bottom = chip_shift(block[far][cut:], -1)
    for d in range(far - 1, 0, -1):
        if d == far - 1:
            up = jnp.concatenate([add(block[d][:cut], top), block[d][cut:]], axis=0)
            down = jnp.concatenate([block[-d][:cut], add(block[-d][cut:], bottom)], axis=0)
        else:
            up = add(block[d], up)
            down = add(block[-d], down)
        up = chip_shift(up, 1)
        down = chip_shift(down, -1)
    f32 = jnp.float32
    return (block[0].astype(f32) + up.astype(f32) + down.astype(f32)).astype(partial.dtype)


def ordered(pieces, me):
    bit = 1
    while bit < len(pieces):
        flag = (me & bit) != 0
        pieces = [jnp.where(flag, pieces[p ^ bit], pieces[p]) for p in range(len(pieces))]
        bit *= 2
    return pieces


def hidden_body(rows, gate_mat, up_mat, out):
    x = rows[...]
    g = jnp.dot(x, gate_mat[0], preferred_element_type=jnp.float32)
    u = jnp.dot(x, up_mat[0], preferred_element_type=jnp.float32)
    out[...] = (g / (1.0 + jnp.exp(-g)) * u).astype(out.dtype)


def hidden_units(flat, w_gate, w_up, first, count, width):
    rows, depth = flat.shape
    weight = pl.BlockSpec((1, depth, width), lambda j: (0, 0, j + first))
    return pl.pallas_call(
        hidden_body,
        grid=(count,),
        in_specs=[pl.BlockSpec((rows, depth), lambda j: (0, 0)), weight, weight],
        out_specs=pl.BlockSpec((rows, width), lambda j: (0, j)),
        out_shape=jax.ShapeDtypeStruct((rows, count * width), flat.dtype),
        cost_estimate=pl.CostEstimate(
            flops=4 * rows * depth * count * width,
            bytes_accessed=4 * depth * count * width,
            transcendentals=0,
        ),
        compiler_params=pltpu.CompilerParams(vmem_limit_bytes=40 << 20),
    )(flat, w_gate, w_up)


def down_body(*refs):
    hiddens, mat, out = refs[:-2], refs[-2], refs[-1]
    total = None
    at = 0
    for h in hiddens:
        part = jnp.dot(
            h[...], mat[0, at : at + h.shape[1], :], preferred_element_type=jnp.float32
        )
        total = part if total is None else total + part
        at += h.shape[1]
    out[...] = total.astype(out.dtype)


def down_product(hiddens, w_down):
    rows = hiddens[0].shape[0]
    _, units, depth = w_down.shape
    width = 512
    return pl.pallas_call(
        down_body,
        grid=(depth // width,),
        in_specs=[pl.BlockSpec(h.shape, lambda j: (0, 0)) for h in hiddens]
        + [pl.BlockSpec((1, units, width), lambda j: (0, 0, j))],
        out_specs=pl.BlockSpec((rows, width), lambda j: (0, j)),
        out_shape=jax.ShapeDtypeStruct((rows, depth), hiddens[0].dtype),
        cost_estimate=pl.CostEstimate(
            flops=2 * rows * depth * units, bytes_accessed=2 * depth * units, transcendentals=0
        ),
        compiler_params=pltpu.CompilerParams(vmem_limit_bytes=40 << 20),
    )(*hiddens, w_down)


def expert(flat, w_gate, w_up, w_down):
    units = w_gate.shape[2]
    width = 256 if units % 256 == 0 else units
    count = units // width
    split = [(0, count // 2), (count // 2, count - count // 2)] if count > 1 else [(0, 1)]
    hiddens = [hidden_units(flat, w_gate, w_up, first, n, width) for first, n in split]
    return down_product(hiddens, w_down)


def attend(queries, keys, values):
    tok_rows, local_width = queries.shape
    kv_width = keys.shape[1]
    local_heads = kv_width // HEAD_WIDTH
    group_width = QUERY_HEADS // KEY_VALUE_HEADS
    score_scale = 1.0 / math.sqrt(HEAD_WIDTH)
    first_pos = lax.axis_index("seq") * tok_rows
    query_pos = first_pos + jnp.arange(tok_rows, dtype=jnp.int32)
    query_grouped = queries.reshape(tok_rows, local_heads, group_width, HEAD_WIDTH)
    both = lax.all_gather(jnp.concatenate([keys, values], axis=1), "seq", axis=0, tiled=True)
    length = both.shape[0]
    key_piece = both[:, :kv_width].reshape(length, local_heads, HEAD_WIDTH)
    value_piece = both[:, kv_width:].reshape(length, local_heads, HEAD_WIDTH)
    key_pos = jnp.arange(length, dtype=jnp.int32)
    scores = (
        jnp.einsum("tkgd,pkd->kgtp", query_grouped, key_piece, preferred_element_type=jnp.float32)
        * score_scale
    )
    causal_mask = key_pos[None, :] <= query_pos[:, None]
    scores = jnp.where(causal_mask, scores, -1e30)
    row_max = jnp.max(scores, axis=-1)
    exp_terms = jnp.where(causal_mask, jnp.exp(scores - row_max[..., None]), 0.0)
    row_sum = jnp.sum(exp_terms, axis=-1)
    weighted = jnp.einsum(
        "kgtp,pkd->kgtd",
        exp_terms.astype(jnp.bfloat16),
        value_piece,
        preferred_element_type=jnp.float32,
    )
    attn = weighted / row_sum[..., None]
    return jnp.transpose(attn, (2, 0, 1, 3)).reshape(tok_rows, local_width)


def shards(queries, keys, values, residual, norm_gain, routes, gates, w_gate, w_up, w_down):
    tok_rows, local_width = queries.shape
    exp_count = lax.axis_size("exp")
    me = lax.axis_index("exp")
    capacity = min(tok_rows, 3 * TOP * tok_rows // (2 * exp_count))
    gain = jnp.concatenate(
        ordered([norm_gain] + [exp_swap(norm_gain, k) for k in range(1, exp_count)], me)
    )
    expert_ids = routes.reshape(tok_rows * TOP)
    relative = expert_ids ^ me
    one_hot = (relative[:, None] == jnp.arange(exp_count, dtype=jnp.int32)[None, :])
    number = jnp.arange(tok_rows * TOP, dtype=jnp.int32)
    earlier = (number[None, :] < number[:, None]).astype(jnp.bfloat16)
    before = jnp.dot(earlier, one_hot.astype(jnp.bfloat16), preferred_element_type=jnp.float32)
    slot_index = jnp.sum(jnp.where(one_hot, before, 0.0), axis=1).astype(jnp.int32)
    dest_slot = (relative * capacity + slot_index).reshape(tok_rows, TOP)
    slots = jnp.arange(exp_count * capacity, dtype=jnp.int32)
    dispatch = jnp.zeros((exp_count * capacity, tok_rows), jnp.float32)
    mixing = jnp.zeros((tok_rows, exp_count * capacity), jnp.float32)
    for t in range(TOP):
        dispatch = dispatch + (slots[:, None] == dest_slot[None, :, t])
        mixing = mixing + jnp.where(dest_slot[:, t, None] == slots[None, :], gates[:, t, None], 0.0)

    attn = attend(queries, keys, values)
    attended = (residual.astype(jnp.float32) + attn).astype(jnp.bfloat16)
    outgoing = jnp.dot(
        dispatch.astype(jnp.bfloat16), attended, preferred_element_type=jnp.float32
    ).astype(jnp.bfloat16)
    pieces = [outgoing[:capacity]]
    for k in range(1, exp_count):
        pieces.append(exp_swap(outgoing[k * capacity : (k + 1) * capacity], k))
    rows = jnp.concatenate(ordered(pieces, me), axis=1).astype(jnp.float32)
    mean_square = jnp.sum(rows * rows, axis=1, keepdims=True) / D
    normed = (rows * lax.rsqrt(mean_square + 1e-05) * gain[None, :]).astype(jnp.bfloat16)

    step = (-(-capacity // CHUNKS) + 7) // 8 * 8
    returned = [[] for _ in range(exp_count)]
    for start in range(0, capacity, step):
        flat = gather_seq(normed[start : min(start + step, capacity)])
        partial = expert(flat, w_gate, w_up, w_down)
        summed = reduce_seq(partial)
        for k in range(exp_count):
            piece = lax.dynamic_slice_in_dim(summed, (me ^ k) * local_width, local_width, axis=1)
            returned[k].append(piece if k == 0 else exp_swap(piece, k))
    returned_rows = jnp.concatenate([piece for pieces in returned for piece in pieces], axis=0)
    expert_mix = jnp.dot(mixing, returned_rows.astype(jnp.float32), precision=lax.Precision.HIGHEST)
    layer_out = (attended.astype(jnp.float32) + expert_mix).astype(jnp.bfloat16)
    return (attended, layer_out)


def solution(mesh):
    in_specs = (
        P("seq", "exp"),
        P("seq", "exp"),
        P("seq", "exp"),
        P("seq", "exp"),
        P("exp"),
        P("seq", None),
        P("seq", None),
        P("exp", None, "seq"),
        P("exp", None, "seq"),
        P("exp", "seq", None),
    )
    out_specs = (P("seq", "exp"), P("seq", "exp"))

    return jax.shard_map(shards, mesh=mesh, in_specs=in_specs, out_specs=out_specs, check_vma=False)
```
